32 devices in a mesh: section: 4 (over z), expert: 4 (over y, x), dp: 2 (over core).
Axes of the slice: x: 2, y: 2, z: 4, core: 2. Of those that a mesh axis runs over, the one named last changes fastest.
Arguments:
- stash: bfloat16 [4, 256, 2048], P('section', 'dp', 'expert'), may hold values from -6 to 6
- cotangent: bfloat16 [4, 256, 2048], P('section', 'dp', 'expert'), may hold values from -6 to 6
- backward_expert_routes: int32 [4, 256, 2], P('section', 'dp'), may hold values from 0 to 3, all different within a row; in each aligned block of 128 rows (0 to 127, 128 to 255, ..., all dimensions but the last counted through in order) at most 80 rows name the same one
- backward_job_lengths: int32 [4, 4], P('section'), may hold values from 1 to 128, 256 in all within a row
- layer_norm_gains: float32 [4, 2048], P('section'), may hold values from 0.25 to 1.75
- router: bfloat16 [4, 2048, 4], P('section'), may hold values from -0.125 to 0.125
- expert_gate_weight: bfloat16 [4, 2048, 28672], P('section', None, ('expert', 'dp')), may hold values from -0.125 to 0.125
- expert_up_weight: bfloat16 [4, 2048, 28672], P('section', None, ('expert', 'dp')), may hold values from -0.125 to 0.125
- expert_down_weight: bfloat16 [4, 28672, 2048], P('section', ('expert', 'dp')), may hold values from -0.0625 to 0.0625
- adapter_down_maps: bfloat16 [4, 2048, 64], P('section', 'expert'), may hold values from -0.125 to 0.125
- adapter_up_maps: bfloat16 [4, 64, 2048], P('section', None, 'expert'), may hold values from -1.5 to 1.5
Outputs:
- handed_back: bfloat16 [4, 256, 2048], P('section', 'dp', 'expert')
- grad_lora_down: float32 [4, 2048, 64], P('section', 'expert')
- grad_lora_up: float32 [4, 64, 2048], P('section', None, 'expert')
The draws below stay inside these ranges and needn't reach their ends.
Inputs may be any that keep to these rules, and one draw needn't show every extreme that they name: `backward_expert_routes`: each row names two different experts. In each aligned block of 128 rows (the tokens of one device) no expert is named more than 80 times. `backward_job_lengths`: each row sums to 256.
All inputs are finite; a program needn't handle non-finite values.
Results may differ from the reference program's by a relative error of at most 0.008.
Values may be sent and summed in bfloat16 or wider, within the bound.
A program may use at most 128 MiB of HBM per device.

```python
import math
import jax
import jax.numpy as jnp
import numpy as np
from jax import lax

MODEL_WIDTH = 2048
FF = 7168
EXPERTS = 4
TOP = 2
ADAPTER_RANK = 16
ADAPTER_JOBS = 4
TOK_DEV = 128
CAP = 80
TOKENS = 256
LAYER_COUNT = 4


def levels(rng, dims, split, low, top_value):
    def one(dim, blocks):
        steps = jax.random.uniform(jax.random.fold_in(jax.random.fold_in(rng, 6), dim), (blocks,), jnp.float32, low / len(split), top_value / len(split))
        return jnp.repeat(jnp.exp(steps), dims[dim] // blocks).reshape((-1,) + (1,) * (len(dims) - dim - 1))

    level = one(*split[0])
    for cut in split[1:]:
        level = level * one(*cut)
    return level


def profile(count, total, reach, lean):
    weights = [(1 << 20) // math.isqrt(rank ** lean) + 1 for rank in range(2, count + 1)]
    spare, given = total - reach - (count - 1), [1] * (count - 1)
    while spare > 0:
        candidates = [i for i in range(count - 1) if given[i] < reach]
        pool, budget = sum([weights[i] for i in candidates]), spare
        for i in candidates:
            extra = min(reach - given[i], max(1, budget * weights[i] // pool), spare)
            given[i] = given[i] + extra
            spare = spare - extra
    return np.array([reach] + given)


def uneven(rng, number_of, total, reach, lean):
    if number_of == 2:
        one = jax.random.randint(rng, (), max(1, total - reach), min(reach, total - 1) + 1)
        return jnp.stack([one, total - one])
    lengths = jnp.asarray(profile(number_of, total, reach, lean), jnp.int32)
    twos = (number_of - 1) // 2
    giver, taker = lengths[1:1 + 2 * twos:2], lengths[2:2 + 2 * twos:2]
    margin = jnp.minimum(giver - 1, reach - taker)
    passed = jax.random.randint(jax.random.fold_in(rng, 1), (twos,), 0, 1 << 20) % (margin + 1)
    lengths = lengths.at[1:1 + 2 * twos:2].set(giver - passed).at[2:2 + 2 * twos:2].set(taker + passed)
    return lengths[jax.random.permutation(jax.random.fold_in(rng, 2), number_of)]


def shared_out(key, own, number, rows, amount, top, limit, slope):
    ranking = jax.random.permutation(key, amount)
    heavy_load, ordinary = shares(amount, rows * top, limit, slope, True), shares(amount, rows * top, limit, slope, False)
    places = jnp.arange(amount)

    def named(sizes, rotation):
        used = int((sizes > 0).sum())
        fixed = max(1, used // 4)
        passed = fixed + (places - fixed + rotation * (used - fixed)) % max(1, amount - fixed)
        return jnp.zeros((amount,), jnp.int32).at[ranking[jnp.where(places < fixed, places, passed)]].set(jnp.asarray(sizes, jnp.int32))

    sizes = jnp.where(number % 4 == 0, named(heavy_load, number // 4), named(ordinary, number - number // 4 - 1))
    mixed = jax.random.permutation(jax.random.fold_in(own, 3), amount)
    donor, taker = mixed[0:amount // 2 * 2:2], mixed[1:amount // 2 * 2:2]
    room = jnp.minimum(sizes[donor] - 1, limit - sizes[taker]) // 2
    room = jnp.where((donor == ranking[0]) | (taker == ranking[0]) | (sizes[taker] == 0), 0, jnp.maximum(room, 0))
    passed = jax.random.randint(jax.random.fold_in(own, 4), (amount // 2,), 0, 1 << 20) % (room + 1)
    sizes = sizes.at[donor].add(-passed).at[taker].add(passed)
    items = jnp.searchsorted(jnp.cumsum(sizes), jnp.arange(rows * top), side="right").astype(jnp.int32)
    grid = items.reshape(top, rows).T
    grid = grid[jax.random.permutation(jax.random.fold_in(own, 1), rows)]
    rotation = jax.random.randint(jax.random.fold_in(own, 2), (rows, 1), 0, top)
    return jnp.take_along_axis(grid, (jnp.arange(top)[None, :] + rotation) % top, axis=1)


def shares(number_of, total, limit, slope, full):
    loads = [(1 << 20) // math.isqrt(standing ** slope) + 1 for standing in range(1, number_of + 1)]
    largest = limit if full else min(limit, max(-(-total // number_of), total * loads[0] // sum(loads)))
    least = 1 if total - largest >= number_of - 1 else 0
    holding, spare = [largest] + [least] * (number_of - 1), total - largest - least * (number_of - 1)
    while spare > 0:
        candidates = [i for i in range(1, number_of) if holding[i] < largest] or [i for i in range(1, number_of) if holding[i] < limit]
        whole, left = sum([loads[i] for i in candidates]), spare
        for i in candidates:
            addition = min(limit - holding[i], max(1, left * loads[i] // whole), spare)
            holding[i] = holding[i] + addition
            spare = spare - addition
    return np.array(holding)


def centred(own_key, extent, scale, bound, pieces=(), held_as=jnp.bfloat16):
    array = scale * jax.random.normal(own_key, extent, jnp.float32)
    if pieces:
        array = array * levels(own_key, extent, pieces, -0.22, 0.18)
    return jnp.clip(array, -bound, bound).astype(held_as)


def setup_inputs(seed: int = 0) -> dict:
    key_of = jax.random.split(jax.random.key(seed), 12)
    stash = centred(key_of[0], (LAYER_COUNT, TOKENS, MODEL_WIDTH), 1.0, 6.0, ((0, 4), (1, 2), (2, 4)))
    cotangent = centred(key_of[1], (LAYER_COUNT, TOKENS, MODEL_WIDTH), 1.0, 6.0, ((0, 4), (1, 2), (2, 4)))
    backward_expert_routes_keys = jax.random.split(jax.random.fold_in(key_of[2], 1), LAYER_COUNT * TOKENS // TOK_DEV)
    backward_expert_routes_turns = jax.random.permutation(jax.random.fold_in(key_of[2], 3), LAYER_COUNT * TOKENS // TOK_DEV)
    backward_expert_routes = jax.vmap(lambda own, number: shared_out(jax.random.fold_in(key_of[2], 2), own, number, TOK_DEV, EXPERTS, TOP, CAP, 2))(backward_expert_routes_keys, backward_expert_routes_turns).reshape((LAYER_COUNT, TOKENS, TOP))
    backward_job_lengths = jax.vmap(lambda own: uneven(own, ADAPTER_JOBS, TOKENS, TOKENS // 2, 2))(jax.random.split(key_of[3], LAYER_COUNT)).reshape((LAYER_COUNT, ADAPTER_JOBS)).astype(jnp.int32)
    layer_norm_gains = jnp.clip(1.0 + 0.15 * jax.random.normal(key_of[4], (LAYER_COUNT, MODEL_WIDTH), jnp.float32), 0.25, 1.75)
    router = centred(key_of[5], (LAYER_COUNT, MODEL_WIDTH, EXPERTS), MODEL_WIDTH ** -0.5, 0.125, ((0, 4),))
    expert_gate_weight = centred(key_of[6], (LAYER_COUNT, MODEL_WIDTH, EXPERTS * FF), MODEL_WIDTH ** -0.5, 0.125, ((0, 4), (2, 8)))
    expert_up_weight = centred(key_of[7], (LAYER_COUNT, MODEL_WIDTH, EXPERTS * FF), MODEL_WIDTH ** -0.5, 0.125, ((0, 4), (2, 8)))
    expert_down_weight = centred(key_of[8], (LAYER_COUNT, EXPERTS * FF, MODEL_WIDTH), FF ** -0.5, 0.0625, ((0, 4), (1, 8)))
    adapter_down_maps = centred(key_of[9], (LAYER_COUNT, MODEL_WIDTH, ADAPTER_JOBS * ADAPTER_RANK), MODEL_WIDTH ** -0.5, 0.125, ((0, 4), (1, 4)))
    adapter_up_maps = centred(key_of[10], (LAYER_COUNT, ADAPTER_JOBS * ADAPTER_RANK, MODEL_WIDTH), ADAPTER_RANK ** -0.5, 1.5, ((0, 4), (2, 4)))
    return {"stash": stash, "cotangent": cotangent, "backward_expert_routes": backward_expert_routes, "backward_job_lengths": backward_job_lengths, "layer_norm_gains": layer_norm_gains, "router": router, "expert_gate_weight": expert_gate_weight, "expert_up_weight": expert_up_weight, "expert_down_weight": expert_down_weight, "adapter_down_maps": adapter_down_maps, "adapter_up_maps": adapter_up_maps}


EPS = 1e-05
ADAPTER_SCALE = 0.5
HIGH = lax.Precision.HIGHEST

def job_columns(job_token_lengths, offset, count):
    ends = jnp.cumsum(job_token_lengths, dtype=jnp.int32)
    position = offset + jnp.arange(count, dtype=jnp.int32)
    owner = lax.optimization_barrier(jnp.sum((ends[None, :] <= position[:, None]).astype(jnp.int32), axis=1, dtype=jnp.int32))
    column_owner = jnp.arange(job_token_lengths.shape[0] * ADAPTER_RANK, dtype=jnp.int32) // ADAPTER_RANK
    return (owner[:, None] == column_owner[None, :]).astype(jnp.float32)

def prepare(whole_batch, norm_gain_vector, router, token_routes):
    expert_values = whole_batch.astype(jnp.float32)
    scale = lax.rsqrt(lax.optimization_barrier(jnp.mean(expert_values * expert_values, axis=1, keepdims=True)) + EPS)
    normalized_input = (expert_values * scale * norm_gain_vector[None, :]).astype(jnp.bfloat16)
    logits = jnp.dot(normalized_input, router, preferred_element_type=jnp.float32)
    labels = jnp.arange(router.shape[1], dtype=jnp.int32)
    first = (token_routes[:, 0:1] == labels[None, :]).astype(jnp.float32)
    second = (token_routes[:, 1:2] == labels[None, :]).astype(jnp.float32)
    upper = jax.nn.sigmoid(lax.optimization_barrier(jnp.sum(first * logits, axis=1)) - lax.optimization_barrier(jnp.sum(second * logits, axis=1)))
    table = upper[:, None] * first + (1.0 - upper)[:, None] * second
    return (expert_values, scale, normalized_input, first, second, upper, table)

def router_grad(gate_grad, first, second, upper):
    spread = lax.optimization_barrier(jnp.sum(first * gate_grad, axis=1)) - lax.optimization_barrier(jnp.sum(second * gate_grad, axis=1))
    delta = spread * upper * (1.0 - upper)
    return delta[:, None] * (first - second)

def layer_backward_pass(whole_batch, adapter_gradient_list, norm_gain_vector, router, expert_gate_weight, expert_up_weight, expert_down_weight, adapter_down_maps, adapter_up_maps, token_routes, job_token_lengths):
    expert_values, scale, normalized_input, first, second, upper, table = prepare(whole_batch, norm_gain_vector, router, token_routes)
    grad_values = adapter_gradient_list.astype(jnp.float32)
    job_mask = job_columns(job_token_lengths, 0, expert_values.shape[0])
    low_rank_rows = (jnp.dot(normalized_input, adapter_down_maps, preferred_element_type=jnp.float32) * job_mask).astype(jnp.bfloat16)
    grad_low_rank = (ADAPTER_SCALE * jnp.dot(adapter_gradient_list, adapter_up_maps.T, preferred_element_type=jnp.float32) * job_mask).astype(jnp.bfloat16)
    up_map_gradient = ADAPTER_SCALE * jnp.dot(low_rank_rows.T, adapter_gradient_list, preferred_element_type=jnp.float32)
    down_map_gradient = jnp.dot(normalized_input.T, grad_low_rank, preferred_element_type=jnp.float32)
    grad_normalized = jnp.dot(grad_low_rank, adapter_down_maps.T, preferred_element_type=jnp.float32)
    gate_terms = []
    for expert in range(EXPERTS):
        lower_col = expert * FF
        wg = expert_gate_weight[:, lower_col:lower_col + FF]
        wu = expert_up_weight[:, lower_col:lower_col + FF]
        wd = expert_down_weight[lower_col:lower_col + FF, :]
        gate = jnp.dot(normalized_input, wg, preferred_element_type=jnp.float32)
        up = jnp.dot(normalized_input, wu, preferred_element_type=jnp.float32)
        sig = jax.nn.sigmoid(gate)
        act = gate * sig
        hidden = (act * up).astype(jnp.bfloat16)
        output = jnp.dot(hidden, wd, preferred_element_type=jnp.float32)
        gate_terms.append(lax.optimization_barrier(jnp.sum(grad_values * output, axis=1)))
        back = jnp.dot(adapter_gradient_list, wd.T, preferred_element_type=jnp.float32)
        d_gate = (back * up * sig * (1.0 + gate * (1.0 - sig))).astype(jnp.bfloat16)
        d_up = (back * act).astype(jnp.bfloat16)
        inner = jnp.dot(d_gate, wg.T, preferred_element_type=jnp.float32) + jnp.dot(d_up, wu.T, preferred_element_type=jnp.float32)
        grad_normalized = grad_normalized + table[:, expert:expert + 1] * inner
    gate_grad = jnp.stack(gate_terms, axis=1)
    d_logit = router_grad(gate_grad, first, second, upper)
    grad_normalized = grad_normalized + jnp.dot(d_logit, router.astype(jnp.float32).T, precision=HIGH)
    weighted = grad_normalized * norm_gain_vector[None, :]
    stat = lax.optimization_barrier(jnp.sum(weighted * expert_values, axis=1, keepdims=True))
    layer_result = grad_values + scale * weighted - expert_values * scale * scale * scale * stat / MODEL_WIDTH
    return (layer_result.astype(jnp.bfloat16), down_map_gradient, up_map_gradient)

def reference(stash, cotangent, backward_expert_routes, backward_job_lengths, layer_norm_gains, router, expert_gate_weight, expert_up_weight, expert_down_weight, adapter_down_maps, adapter_up_maps):

    def single_layer_tick(items):
        x_stash, adapter_gradient_list, b_routes, b_lengths, norm_gain_vector, route_w, wg, wu, wd, a_map, b_map = items
        return layer_backward_pass(x_stash, adapter_gradient_list, norm_gain_vector, route_w, wg, wu, wd, a_map, b_map, b_routes, b_lengths)
    backward_outputs, down_map_gradient, up_map_gradient = lax.map(single_layer_tick, (stash, cotangent, backward_expert_routes, backward_job_lengths, layer_norm_gains, router, expert_gate_weight, expert_up_weight, expert_down_weight, adapter_down_maps, adapter_up_maps))
    return (jnp.roll(backward_outputs, -1, axis=0), down_map_gradient, up_map_gradient)
```

```python
import functools

import jax
import jax.numpy as jnp
from jax import lax
from jax.experimental import pallas as pl
from jax.experimental.pallas import tpu as pltpu
from jax.sharding import PartitionSpec as P

CAP = 80

EPS = 1e-05
ADAPTER_SCALE = 0.5
MESH = pl.DeviceIdType.MESH
VMEM_LIMIT = 67_043_328
LANES = 128
DEPTH = 2
TILES = (1792, 896, 512, 256, 128)
LAST = (((1,), (1,)), ((), ()))
FIRST = (((0,), (0,)), ((), ()))


def greet(targets):
    barrier = pltpu.get_barrier_semaphore()
    for target in targets:
        pl.semaphore_signal(barrier, inc=1, device_id=target, device_id_type=MESH)
    pl.semaphore_wait(barrier, len(targets))


def paired(me, k, n):
    out, bit = me, 1
    while bit < n:
        if k & bit:
            out = out + bit * (1 - 2 * lax.rem(me // bit, 2))
        bit *= 2
    return out


def tick_kernel(
    n, per, experts, sections,
    x_ref, g_ref, route_ref, len_ref, gain_ref, router_ref, down_ref, up_ref, wg_hbm, wu_hbm, wd_hbm,
    back_out, pd_out, pu_out,
    wg_v, wu_v, wd_v, rows_in, rows_ref, select_ref, stats_ref, lows_ref, stats_in, lows_in,
    gate_acc, up_acc, back_acc, dg_ref, du_ref, ssq, gsum, ssum, vec_ref, dn_ref,
    pdn, pvec, pd_ref, pu_ref, ppd, ppu, sendbuf, landing, result, turn,
    ws, rs, rr, fs, fr, ss, sr, ls, lr, own, qs, qr, ps, pr, es, er, zs, zr,
):
    me = lax.axis_index("expert")
    core = lax.axis_index("dp")
    sec = lax.axis_index("section")
    other = 1 - core
    partner = {"dp": other}
    ahead = {"section": lax.rem(sec + sections - 1, sections)}
    behind = {"section": lax.rem(sec + 1, sections)}
    peers = [paired(me, k, n) for k in range(n)]
    count, width = x_ref.shape
    cap = select_ref.shape[1]
    hidden = wg_v.shape[2]
    f32, bf16 = jnp.float32, jnp.bfloat16

    def weights(k):
        cols = pl.ds(pl.multiple_of(peers[k] * width, LANES), width)
        return [
            pltpu.make_async_copy(wg_hbm.at[0, cols, :], wg_v.at[k], ws.at[k, 0]),
            pltpu.make_async_copy(wu_hbm.at[0, cols, :], wu_v.at[k], ws.at[k, 1]),
            pltpu.make_async_copy(wd_hbm.at[0, :, cols], wd_v.at[k], ws.at[k, 2]),
        ]

    loads = [weights(k) for k in range(n)]
    for k in range(min(DEPTH, n)):
        for copy in loads[k]:
            copy.start()

    def send(src, dst, a, b, k, target):
        copy = pltpu.make_async_remote_copy(
            src_ref=src, dst_ref=dst, send_sem=a.at[k], recv_sem=b.at[k],
            device_id=target, device_id_type=MESH,
        )
        copy.start()
        return copy

    line = lax.broadcasted_iota(jnp.int32, (8, count), 0)
    first = (route_ref[0:1, :] == line).astype(f32)
    second = (route_ref[1:2, :] == line).astype(f32)
    member = first + second
    before = (
        lax.broadcasted_iota(jnp.int32, (count, count), 0)
        < lax.broadcasted_iota(jnp.int32, (count, count), 1)
    ).astype(bf16)
    rank = jnp.dot(member.astype(bf16), before, preferred_element_type=f32)
    place = jnp.where(member > 0, rank, -1.0)
    slot = lax.broadcasted_iota(jnp.int32, (cap, count), 0).astype(f32)
    x, g = x_ref[...], g_ref[...]
    for e in range(experts):
        chosen = (place[e:e + 1, :] == slot).astype(bf16)
        select_ref[e] = chosen
        rows_ref[e, :, :width] = jnp.dot(chosen, x, preferred_element_type=f32).astype(bf16)
        rows_ref[e, :, width:] = jnp.dot(chosen, g, preferred_element_type=f32).astype(bf16)

    greet([{"expert": peer} for peer in peers[1:]] + [partner, ahead, behind])
    mine = pl.ds(pl.multiple_of(core * cap, 16), cap)
    home = rows_ref.at[me // per]
    forwards = [send(home, rows_in.at[0, mine], fs, fr, 0, partner)]
    rows = [
        send(rows_ref.at[peers[k] // per], rows_in.at[k, mine], rs, rr, k - 1, {"expert": peers[k]})
        for k in range(1, n)
    ]
    kept = pltpu.make_async_copy(home, rows_in.at[0, mine], own.at[0])
    kept.start()

    xf = x.astype(f32)
    features = pl.ds(pl.multiple_of(me * width, LANES), width)
    gained = (xf * gain_ref[:, features]).astype(bf16)
    router = jnp.concatenate(
        [router_ref[:, features].astype(f32), jnp.zeros((8 - experts, width), f32)], axis=0
    )
    raw = lax.dot_general(router.astype(bf16), gained, LAST, preferred_element_type=f32)
    square = lax.dot_general(
        jnp.ones((8, width), f32), xf * xf, LAST,
        precision=lax.Precision.HIGHEST, preferred_element_type=f32,
    )
    stats_ref[...] = jnp.where(line < experts, raw, square)
    lows_ref[...] = jnp.concatenate(
        [
            lax.dot_general(gained, down_ref[...], LAST, preferred_element_type=f32),
            lax.dot_general(g, up_ref[...], LAST, preferred_element_type=f32),
        ],
        axis=1,
    ).astype(bf16)
    small = []
    for k in range(1, n):
        target = {"expert": peers[k]}
        small.append(send(stats_ref, stats_in.at[k - 1], ss, sr, k - 1, target))
        small.append(send(lows_ref, lows_in.at[k - 1], ls, lr, k - 1, target))

    def pass_on(k):
        rows[k - 1].wait_recv()
        landed = rows_in.at[k, mine]
        forwards.append(send(landed, landed, fs, fr, k, partner))

    tile = next(t for t in TILES if hidden % t == 0)
    act_tile = next(t for t in (512, 256, 128) if hidden % t == 0)
    kept.wait()
    for k in range(n):
        if k == 1:
            for q in range(1, min(3, n)):
                pass_on(q)
        forwards[k].wait()
        features = pl.ds(pl.multiple_of(peers[k] * width, LANES), width)
        xk = rows_in[k, :, :width].astype(f32)
        part = jnp.sum(xk * xk, axis=1, keepdims=True)
        if k == 0:
            ssq[...] = jnp.broadcast_to(part, ssq.shape)
        else:
            ssq[...] += part
        xk = (xk * gain_ref[:, features]).astype(bf16)
        gk = rows_in[k, :, width:]
        loads[k][0].wait()
        if k + DEPTH < n:
            for copy in loads[k + DEPTH]:
                copy.start()
        if k < n - 1:
            for acc, w, load in ((gate_acc, wg_v, None), (up_acc, wu_v, 1), (back_acc, wd_v, 2)):
                if load is not None:
                    loads[k][load].wait()
                if load == 2 and 3 <= k + 1:
                    pass_on(k + 1)
                for t in range(hidden // tile):
                    c = slice(t * tile, (t + 1) * tile)
                    if load == 2:
                        p = lax.dot_general(gk, w[k, c, :], LAST, preferred_element_type=f32)
                    else:
                        p = jnp.dot(xk, w[k, :, c], preferred_element_type=f32)
                    if k == 0:
                        acc[:, c] = p
                    else:
                        acc[:, c] += p
        else:
            loads[k][1].wait()
            loads[k][2].wait()
            scale = lax.rsqrt(ssq[:, 0:1] / (n * width) + EPS)
            gsum[...] = jnp.zeros_like(gsum)
            ssum[...] = jnp.zeros_like(ssum)
            for t in range(hidden // act_tile):
                c = slice(t * act_tile, (t + 1) * act_tile)
                gate = jnp.dot(xk, wg_v[k, :, c], preferred_element_type=f32)
                up = jnp.dot(xk, wu_v[k, :, c], preferred_element_type=f32)
                back = lax.dot_general(gk, wd_v[k, c, :], LAST, preferred_element_type=f32)
                gate = (gate + gate_acc[:, c]) * scale
                up = (up + up_acc[:, c]) * scale
                back = back + back_acc[:, c]
                sig = jax.nn.sigmoid(gate)
                act = gate * sig
                d_up = back * act
                d_gate = back * up * sig * (1.0 + gate * (1.0 - sig))
                dg_ref[:, c] = d_gate.astype(bf16)
                du_ref[:, c] = d_up.astype(bf16)
                p = d_up * up
                q = d_gate * gate + p
                for j in range(act_tile // LANES):
                    l = slice(j * LANES, (j + 1) * LANES)
                    gsum[...] += p[:, l]
                    ssum[...] += q[:, l]
    lane = lax.broadcasted_iota(jnp.int32, gsum.shape, 1)
    vec_ref[...] = jnp.where(
        lane % 2 == 0,
        jnp.sum(gsum[...], axis=1, keepdims=True),
        jnp.sum(ssum[...], axis=1, keepdims=True),
    )
    theirs = pl.ds(pl.multiple_of(other * cap, 8), cap)
    ours = pl.ds(pl.multiple_of(core * cap, 8), cap)
    shared = [send(vec_ref.at[theirs], pvec, qs, qr, 0, partner)]

    sub = next(t for t in (256, 128) if width % t == 0)
    order = list(range(n - 1, -1, -1))
    blocks, sent, box = {}, {}, {}

    def finish(k):
        blocks[k].wait()
        if not box:
            shared[0].wait()
            v = vec_ref[ours, :] + pvec[...]
            high = v.astype(bf16)
            rest = (v - high.astype(f32)).astype(bf16)
            lane = lax.broadcasted_iota(jnp.int32, v.shape, 1)
            box["packed"] = jnp.where(lane < 2, high.astype(f32), rest.astype(f32)).astype(bf16)
            sendbuf[0, :, width:] = box["packed"]
        sendbuf[k, :, :width] = (dn_ref[k, ours, :] + pdn[k]).astype(bf16)
        if k:
            sendbuf[k, :, width:] = sendbuf[0, :, width:]
            sent[k] = send(
                sendbuf.at[k], landing.at[k - 1], es, er, k - 1, {"expert": peers[k]}
            )

    for i, k in enumerate(order):
        for j in range(width // sub):
            c = slice(j * sub, (j + 1) * sub)
            dn_ref[k, :, c] = lax.dot_general(
                dg_ref[...], wg_v[k, c, :], LAST, preferred_element_type=f32
            ) + lax.dot_general(du_ref[...], wu_v[k, c, :], LAST, preferred_element_type=f32)
            if j == 0 and i > 0:
                finish(order[i - 1])
        blocks[k] = send(dn_ref.at[k, theirs], pdn.at[k], ps, pr, k, partner)

    for copy in small:
        copy.wait()
    stat_rows, low_all = stats_ref[...], lows_ref[...].astype(f32)
    for k in range(1, n):
        stat_rows = stat_rows + stats_in[k - 1]
        low_all = low_all + lows_in[k - 1].astype(f32)
    scale_row = lax.rsqrt(stat_rows[experts:experts + 1, :] / (n * width) + EPS)
    sign_rows = first - second
    spread_row = jnp.sum(
        jnp.where(line < experts, sign_rows * stat_rows, 0.0), axis=0, keepdims=True
    )
    upper = jax.nn.sigmoid(spread_row * scale_row)
    turn[...] = jnp.zeros_like(turn)
    turn[0:8, :] = upper * first + (1.0 - upper) * second
    turn[8:16, :] = sign_rows
    turn[16:17, :] = upper * (1.0 - upper)
    turn[17:18, :] = scale_row
    turn[18:19, :] = spread_row
    token = turn[...].T
    column = lambda i: token[:, i:i + 1]
    delta_of, scale, raw_spread = column(16), column(17), column(18)
    x = x_ref[...].astype(f32)
    ranks = down_ref.shape[0]
    raw_low, g_low = low_all[:, :ranks], low_all[:, ranks:]
    jobs = len_ref.shape[1]
    position = core * count + lax.broadcasted_iota(jnp.int32, (count, ranks), 0)
    owner = jnp.zeros((count, ranks), jnp.int32)
    end = jnp.zeros((1, 1), jnp.int32)
    for j in range(jobs):
        end = end + len_ref[0:1, j:j + 1]
        owner = owner + (end <= position).astype(jnp.int32)
    mask = (
        owner == lax.broadcasted_iota(jnp.int32, (count, ranks), 1) // (ranks // jobs)
    ).astype(f32)
    low = (raw_low * scale * mask).astype(bf16)
    d_low = (ADAPTER_SCALE * g_low * mask).astype(bf16)
    gain = gain_ref[:, pl.ds(pl.multiple_of(me * width, LANES), width)]
    normed = (x * scale * gain).astype(bf16)
    pd_ref[...] = lax.dot_general(d_low, normed, FIRST, preferred_element_type=f32)
    pu_ref[...] = ADAPTER_SCALE * lax.dot_general(low, g_ref[...], FIRST, preferred_element_type=f32)
    shared.append(send(pd_ref, ppd, qs, qr, 1, partner))
    shared.append(send(pu_ref, ppu, qs, qr, 2, partner))
    low_stat = jnp.sum(d_low.astype(f32) * raw_low, axis=1, keepdims=True)
    spread = jnp.zeros((count, 1), f32)
    stat = jnp.zeros((count, 1), f32)
    total = jnp.dot(d_low, down_ref[...], preferred_element_type=f32)

    def add(k, block, total, spread, stat):
        expert = peers[k] // per
        gate, sign = jnp.zeros((count, 1), f32), jnp.zeros((count, 1), f32)
        for e in range(experts):
            mark = (expert == e).astype(f32)
            gate += mark * column(e)
            sign += mark * column(8 + e)
        picked = lax.dot_general(select_ref[expert], block, FIRST, preferred_element_type=f32)
        tail = picked[:, width:]
        spread = spread + sign * (tail[:, 0:1] + tail[:, 2:3])
        stat = stat + gate * (tail[:, 1:2] + tail[:, 3:4])
        return total + gate * picked[:, :width], spread, stat

    finish(0)
    total, spread, stat = add(0, sendbuf[0], total, spread, stat)
    for k in order[:-1]:
        sent[k].wait()
        total, spread, stat = add(k, landing[k - 1], total, spread, stat)
    delta = spread * delta_of
    router = router_ref[:, pl.ds(pl.multiple_of(me * width, LANES), width)].astype(f32)
    for e in range(experts):
        total = total + (delta * column(8 + e)) * router[e:e + 1, :]
    stat = stat / scale + low_stat + delta * raw_spread
    weighted = total * gain
    out = g_ref[...].astype(f32) + scale * weighted - x * (
        scale * scale * scale * stat / (n * width)
    )
    result[...] = out.astype(bf16)
    handed = send(result, back_out, zs, zr, 0, ahead)
    for k in range(1, n):
        rows[k - 1].wait_send()
    shared[1].wait()
    pd_out[...] = pd_ref[...] + ppd[...]
    shared[2].wait()
    pu_out[...] = pu_ref[...] + ppu[...]
    handed.wait()


def settle_kernel(*refs):
    half = len(refs) // 2
    for src, dst in zip(refs[:half], refs[half:]):
        dst[...] = src[...]


def tick(n, per, shards, sections, x, g, routes, lengths, gains, router, down, up, wg, wu, wd):
    count, width = x.shape
    experts = router.shape[0]
    hidden = wg.shape[2]
    ranks = down.shape[0]
    slots = shards * CAP
    f32, bf16 = jnp.float32, jnp.bfloat16
    vmem = pl.BlockSpec(memory_space=pltpu.VMEM)
    hbm = pl.BlockSpec(memory_space=pl.ANY)
    dma = pltpu.SemaphoreType.DMA
    outs = (
        jax.ShapeDtypeStruct((count, width), bf16),
        jax.ShapeDtypeStruct((ranks, width), f32),
        jax.ShapeDtypeStruct((ranks, width), f32),
    )
    values = pl.pallas_call(
        functools.partial(tick_kernel, n, per, experts, sections),
        out_shape=outs,
        in_specs=[vmem] * 8 + [hbm] * 3,
        out_specs=(vmem,) * 3,
        scratch_shapes=[
            pltpu.VMEM((n, width, hidden), bf16),
            pltpu.VMEM((n, width, hidden), bf16),
            pltpu.VMEM((n, hidden, width), bf16),
            pltpu.VMEM((n, slots, 2 * width), bf16),
            pltpu.VMEM((experts, CAP, 2 * width), bf16),
            pltpu.VMEM((experts, CAP, count), bf16),
            pltpu.VMEM((8, count), f32),
            pltpu.VMEM((count, 2 * ranks), bf16),
            pltpu.VMEM((n - 1, 8, count), f32),
            pltpu.VMEM((n - 1, count, 2 * ranks), bf16),
            pltpu.VMEM((slots, hidden), f32),
            pltpu.VMEM((slots, hidden), f32),
            pltpu.VMEM((slots, hidden), f32),
            pltpu.VMEM((slots, hidden), bf16),
            pltpu.VMEM((slots, hidden), bf16),
            pltpu.VMEM((slots, LANES), f32),
            pltpu.VMEM((slots, LANES), f32),
            pltpu.VMEM((slots, LANES), f32),
            pltpu.VMEM((slots, LANES), f32),
            pltpu.VMEM((n, slots, width), f32),
            pltpu.VMEM((n, CAP, width), f32),
            pltpu.VMEM((CAP, LANES), f32),
            pltpu.VMEM((ranks, width), f32),
            pltpu.VMEM((ranks, width), f32),
            pltpu.VMEM((ranks, width), f32),
            pltpu.VMEM((ranks, width), f32),
            pltpu.VMEM((n, CAP, width + LANES), bf16),
            pltpu.VMEM((n - 1, CAP, width + LANES), bf16),
            pltpu.VMEM((count, width), bf16),
            pltpu.VMEM((LANES, count), f32),
            dma((n, 3)),
            dma((n - 1,)), dma((n - 1,)), dma((n,)), dma((n,)),
            dma((n - 1,)), dma((n - 1,)), dma((n - 1,)), dma((n - 1,)),
            dma((1,)), dma((3,)), dma((3,)), dma((n,)), dma((n,)),
            dma((n - 1,)), dma((n - 1,)), dma((1,)), dma((1,)),
        ],
        compiler_params=pltpu.CompilerParams(
            collective_id=0, has_side_effects=True, vmem_limit_bytes=VMEM_LIMIT
        ),
    )(x, g, routes, lengths, gains, router, down, up, wg, wu, wd)
    return pl.pallas_call(
        settle_kernel, out_shape=outs, in_specs=[vmem] * 3, out_specs=(vmem,) * 3
    )(*values)


def body(
    stash,
    cotangent,
    backward_expert_routes,
    backward_job_lengths,
    layer_norm_gains,
    router,
    expert_gate_weight,
    expert_up_weight,
    expert_down_weight,
    adapter_down_maps,
    adapter_up_maps,
):
    n = lax.axis_size("expert")
    shards = lax.axis_size("dp")
    sections = lax.axis_size("section")
    per = n // router.shape[2]
    handed_back, down_grad, up_grad = tick(
        n, per, shards, sections, stash[0], cotangent[0], backward_expert_routes[0].T,
        backward_job_lengths, layer_norm_gains, router[0].T, adapter_down_maps[0].T,
        adapter_up_maps[0], expert_gate_weight, expert_up_weight, expert_down_weight,
    )
    return (handed_back[None], down_grad.T[None], up_grad[None])


def solution(mesh):
    return jax.shard_map(
        body,
        mesh=mesh,
        in_specs=(
            P("section", "dp", "expert"),
            P("section", "dp", "expert"),
            P("section", "dp", None),
            P("section", None),
            P("section", None),
            P("section", None, None),
            P("section", None, ("expert", "dp")),
            P("section", None, ("expert", "dp")),
            P("section", ("expert", "dp"), None),
            P("section", "expert", None),
            P("section", None, "expert"),
        ),
        out_specs=(
            P("section", "dp", "expert"),
            P("section", "expert", None),
            P("section", None, "expert"),
        ),
        check_vma=False,
    )
```

```python
import functools

import jax
import jax.numpy as jnp
from jax import lax
from jax.experimental import pallas as pl
from jax.experimental.pallas import tpu as pltpu
from jax.sharding import PartitionSpec as P

CAP = 80

EPS = 1e-05
ADAPTER_SCALE = 0.5
MESH = pl.DeviceIdType.MESH
VMEM_LIMIT = 63 * 1024 * 1024
LANES = 128
DEPTH = 6
TILES = (1792, 896, 512, 256, 128)
ACT_TILES = (512, 256, 128)
LAST = (((1,), (1,)), ((), ()))
FIRST = (((0,), (0,)), ((), ()))


def paired(me, k, n):
    out, bit = me, 1
    while bit < n:
        if k & bit:
            out = out + bit * (1 - 2 * lax.rem(me // bit, 2))
        bit *= 2
    return out


def tick_kernel(
    n, per, experts, sections,
    x_ref, g_ref, route_ref, len_ref, gain_ref, router_ref, down_ref, up_ref, wg_hbm, wu_hbm, wd_hbm,
    back_out, pd_out, pu_out,
    wg_v, wu_v, wd_v, xs_in, gs_in, xs_ref, gs_ref, select_ref, stats_ref, lows_ref, stats_in, lows_in,
    gate_acc, up_acc, back_acc, dg_ref, du_ref, ssq, gsum, ssum, vec_ref, dn_ref,
    pdn, pvec, vsend, vec_in, pd_ref, pu_ref, ppd, ppu, sendbuf, landing, out_ref, result, turn,
    ws, xs_s, xs_r, gs_s, gs_r, xfs, xfr, gfs, gfr, ss, sr, ls, lr, own, qs, qr, vs, vr, ps, pr,
    es, er, zs, zr,
):
    me = lax.axis_index("expert")
    core = lax.axis_index("dp")
    sec = lax.axis_index("section")
    other = 1 - core
    partner = {"dp": other}
    ahead = {"section": lax.rem(sec + sections - 1, sections)}
    behind = {"section": lax.rem(sec + 1, sections)}
    peers = [paired(me, k, n) for k in range(n)]
    count, width = x_ref.shape
    cap = select_ref.shape[1]
    hidden = wg_v.shape[2]
    f32, bf16 = jnp.float32, jnp.bfloat16

    def weights(k):
        cols = pl.ds(pl.multiple_of(peers[k] * width, LANES), width)
        return [
            pltpu.make_async_copy(wg_hbm.at[0, cols, :], wg_v.at[k], ws.at[k, 0]),
            pltpu.make_async_copy(wu_hbm.at[0, cols, :], wu_v.at[k], ws.at[k, 1]),
            pltpu.make_async_copy(wd_hbm.at[0, :, cols], wd_v.at[k], ws.at[k, 2]),
        ]

    inner = list(range(1, n - 1))
    groups = [inner[i:i + 2] for i in range(0, len(inner), 2)] + [[n - 1]]
    blocks_of = [weights(k) for k in range(n)]
    loads = list(blocks_of[0])
    for group in groups:
        loads += [blocks_of[k][i] for k in group for i in (0, 1)] + [blocks_of[k][2] for k in group]
    for copy in loads[:DEPTH]:
        copy.start()
    loaded = [0]

    def load(count):
        for _ in range(count):
            loads[loaded[0]].wait()
            if loaded[0] + DEPTH < len(loads):
                loads[loaded[0] + DEPTH].start()
            loaded[0] += 1

    neighbours = [{"expert": peer} for peer in peers[1:]] + [partner, ahead, behind]
    barrier = pltpu.get_barrier_semaphore()
    for target in neighbours:
        pl.semaphore_signal(barrier, inc=1, device_id=target, device_id_type=MESH)

    def send(src, dst, a, b, k, target):
        copy = pltpu.make_async_remote_copy(
            src_ref=src, dst_ref=dst, send_sem=a.at[k], recv_sem=b.at[k],
            device_id=target, device_id_type=MESH,
        )
        copy.start()
        return copy

    line = lax.broadcasted_iota(jnp.int32, (8, count), 0)
    first = (route_ref[0:1, :] == line).astype(f32)
    second = (route_ref[1:2, :] == line).astype(f32)
    member = first + second
    before = (
        lax.broadcasted_iota(jnp.int32, (count, count), 0)
        < lax.broadcasted_iota(jnp.int32, (count, count), 1)
    ).astype(bf16)
    rank = jnp.dot(member.astype(bf16), before, preferred_element_type=f32)
    place = jnp.where(member > 0, rank, -1.0)
    slot = lax.broadcasted_iota(jnp.int32, (cap, count), 0).astype(f32)
    x, g = x_ref[...], g_ref[...]
    for e in range(experts):
        chosen = (place[e:e + 1, :] == slot).astype(bf16)
        select_ref[e] = chosen
        xs_ref[e] = jnp.dot(chosen, x, preferred_element_type=f32).astype(bf16)
        gs_ref[e] = jnp.dot(chosen, g, preferred_element_type=f32).astype(bf16)

    pl.semaphore_wait(barrier, len(neighbours))
    mine = pl.ds(pl.multiple_of(core * cap, 16), cap)
    home = me // per
    xs_on = [send(xs_ref.at[home], xs_in.at[0, mine], xfs, xfr, 0, partner)]
    gs_on = [send(gs_ref.at[home], gs_in.at[0, mine], gfs, gfr, 0, partner)]
    xs, gs = {}, {}
    for group in groups:
        for k in group:
            xs[k] = send(
                xs_ref.at[peers[k] // per], xs_in.at[k, mine], xs_s, xs_r, k - 1, {"expert": peers[k]}
            )
        for k in group:
            gs[k] = send(
                gs_ref.at[peers[k] // per], gs_in.at[k, mine], gs_s, gs_r, k - 1, {"expert": peers[k]}
            )
    kept = [
        pltpu.make_async_copy(xs_ref.at[home], xs_in.at[0, mine], own.at[0]),
        pltpu.make_async_copy(gs_ref.at[home], gs_in.at[0, mine], own.at[1]),
    ]
    for copy in kept:
        copy.start()

    xf = x.astype(f32)
    features = pl.ds(pl.multiple_of(me * width, LANES), width)
    gained = (xf * gain_ref[:, features]).astype(bf16)
    router = jnp.concatenate(
        [router_ref[:, features].astype(f32), jnp.zeros((8 - experts, width), f32)], axis=0
    )
    raw = lax.dot_general(router.astype(bf16), gained, LAST, preferred_element_type=f32)
    square = lax.dot_general(
        jnp.ones((8, width), f32), xf * xf, LAST,
        precision=lax.Precision.HIGHEST, preferred_element_type=f32,
    )
    stats_ref[...] = jnp.where(line < experts, raw, square)
    lows_ref[...] = jnp.concatenate(
        [
            lax.dot_general(gained, down_ref[...], LAST, preferred_element_type=f32),
            lax.dot_general(g, up_ref[...], LAST, preferred_element_type=f32),
        ],
        axis=1,
    ).astype(bf16)
    small = []
    for k in range(1, n):
        target = {"expert": peers[k]}
        small.append(send(stats_ref, stats_in.at[k - 1], ss, sr, k - 1, target))
        small.append(send(lows_ref, lows_in.at[k - 1], ls, lr, k - 1, target))

    def pass_on(group, arrived, buffer, onward, a, b):
        for k in group:
            arrived[k].wait_recv()
            landed = buffer.at[k, mine]
            onward.append(send(landed, landed, a, b, k, partner))

    pass_x = lambda group: pass_on(group, xs, xs_in, xs_on, xfs, xfr)
    pass_g = lambda group: pass_on(group, gs, gs_in, gs_on, gfs, gfr)

    tile = next(t for t in TILES if hidden % t == 0)

    def add_to(acc, k, c, p):
        if k == 0:
            acc[:, c] = p
        else:
            acc[:, c] += p

    def scaled(k):
        xs_on[k].wait()
        xk = xs_in[k].astype(f32)
        part = jnp.sum(xk * xk, axis=1, keepdims=True)
        if k == 0:
            ssq[...] = jnp.broadcast_to(part, ssq.shape)
        else:
            ssq[...] += part
        features = pl.ds(pl.multiple_of(peers[k] * width, LANES), width)
        return (xk * gain_ref[:, features]).astype(bf16)

    def forth(k):
        load(2)
        xk = scaled(k)
        for t in range(hidden // tile):
            c = slice(t * tile, (t + 1) * tile)
            add_to(gate_acc, k, c, jnp.dot(xk, wg_v[k, :, c], preferred_element_type=f32))
            add_to(up_acc, k, c, jnp.dot(xk, wu_v[k, :, c], preferred_element_type=f32))

    def back_from(k):
        load(1)
        gs_on[k].wait()
        for t in range(hidden // tile):
            c = slice(t * tile, (t + 1) * tile)
            add_to(back_acc, k, c, lax.dot_general(
                gs_in[k], wd_v[k, c, :], LAST, preferred_element_type=f32
            ))

    for copy in kept:
        copy.wait()
    forth(0)
    back_from(0)
    pass_x(groups[0])
    for i, group in enumerate(groups[:-1]):
        for j, k in enumerate(group):
            forth(k)
            if j == 0:
                pass_g(group)
        pass_x(groups[i + 1])
        for k in group:
            back_from(k)
    k = n - 1
    pass_g(groups[-1])
    load(2)
    xk = scaled(k)
    load(1)
    gs_on[k].wait()
    scale = lax.rsqrt(ssq[:, 0:1] / (n * width) + EPS)
    gk = gs_in[k]
    gate_sum = jnp.zeros(gsum.shape, f32)
    stat_sum = jnp.zeros(gsum.shape, f32)
    act_tile = next(t for t in ACT_TILES if hidden % t == 0)
    for t in range(hidden // act_tile):
        c = slice(t * act_tile, (t + 1) * act_tile)
        gate = jnp.dot(xk, wg_v[k, :, c], preferred_element_type=f32)
        up = jnp.dot(xk, wu_v[k, :, c], preferred_element_type=f32)
        back = lax.dot_general(gk, wd_v[k, c, :], LAST, preferred_element_type=f32)
        gate = (gate + gate_acc[:, c]) * scale
        up = (up + up_acc[:, c]) * scale
        back = back + back_acc[:, c]
        sig = jax.nn.sigmoid(gate)
        act = gate * sig
        both = back * up
        d_gate = both * (sig + act * (1.0 - sig))
        dg_ref[:, c] = d_gate.astype(bf16)
        du_ref[:, c] = (back * act).astype(bf16)
        p, q = both * act, d_gate * gate
        for j in range(act_tile // LANES):
            l = slice(j * LANES, (j + 1) * LANES)
            gate_sum += p[:, l]
            stat_sum += q[:, l]
    gsum[...] = gate_sum
    ssum[...] = stat_sum
    theirs = pl.ds(pl.multiple_of(other * cap, 8), cap)
    ours = pl.ds(pl.multiple_of(core * cap, 8), cap)

    order = list(range(n - 1, -1, -1))
    shared, halves, sent, told = [], {}, {}, []

    def finish(k):
        halves[k].wait()
        sendbuf[k] = (dn_ref[k, ours, :] + pdn[k]).astype(bf16)
        if k:
            sent[k] = send(sendbuf.at[k], landing.at[k - 1], es, er, k - 1, {"expert": peers[k]})

    def tell():
        shared[0].wait()
        v = vec_ref[ours, :] + pvec[...]
        high = v.astype(bf16)
        rest = (v - high.astype(f32)).astype(bf16)
        lane = lax.broadcasted_iota(jnp.int32, v.shape, 1)
        vsend[...] = jnp.where(lane < 2, high.astype(f32), rest.astype(f32)).astype(bf16)
        for k in range(1, n):
            told.append(send(vsend, vec_in.at[k - 1], vs, vr, k - 1, {"expert": peers[k]}))

    sub = next(t for t in (256, 128) if width % t == 0)

    def gradient(k, d_ref, w_ref, fresh):
        for j in range(width // sub):
            c = slice(j * sub, (j + 1) * sub)
            p = lax.dot_general(d_ref[...], w_ref[k, c, :], LAST, preferred_element_type=f32)
            if fresh:
                dn_ref[k, :, c] = p
            else:
                dn_ref[k, :, c] += p

    for i, k in enumerate(order):
        if k:
            for j in range(width // sub):
                c = slice(j * sub, (j + 1) * sub)
                dn_ref[k, :, c] = lax.dot_general(
                    dg_ref[...], wg_v[k, c, :], LAST, preferred_element_type=f32
                ) + lax.dot_general(du_ref[...], wu_v[k, c, :], LAST, preferred_element_type=f32)
        else:
            gradient(k, dg_ref, wg_v, True)
            finish(order[i - 1])
            gradient(k, du_ref, wu_v, False)
        if i == 0:
            gate_sum, stat_sum = gsum[...], ssum[...]
            total = jnp.sum(gate_sum, axis=1, keepdims=True)
            lane = lax.broadcasted_iota(jnp.int32, gsum.shape, 1)
            vec_ref[...] = jnp.where(
                lane % 2 == 0, total, total + jnp.sum(stat_sum, axis=1, keepdims=True)
            )
            shared.append(send(vec_ref.at[theirs], pvec, qs, qr, 0, partner))
        halves[k] = send(dn_ref.at[k, theirs], pdn.at[k], ps, pr, k, partner)
        if i == 1:
            tell()
        if 0 < i and k:
            finish(order[i - 1])

    for copy in small:
        copy.wait()
    stat_rows, low_all = stats_ref[...], lows_ref[...].astype(f32)
    for k in range(1, n):
        stat_rows = stat_rows + stats_in[k - 1]
        low_all = low_all + lows_in[k - 1].astype(f32)
    scale_row = lax.rsqrt(stat_rows[experts:experts + 1, :] / (n * width) + EPS)
    sign_rows = first - second
    spread_row = jnp.sum(
        jnp.where(line < experts, sign_rows * stat_rows, 0.0), axis=0, keepdims=True
    )
    upper = jax.nn.sigmoid(spread_row * scale_row)
    turn[...] = jnp.zeros_like(turn)
    turn[0:8, :] = upper * first + (1.0 - upper) * second
    turn[8:16, :] = sign_rows
    turn[16:17, :] = upper * (1.0 - upper)
    turn[17:18, :] = scale_row
    turn[18:19, :] = spread_row
    token = turn[...].T
    column = lambda i: token[:, i:i + 1]
    delta_of, scale, raw_spread = column(16), column(17), column(18)
    x = x_ref[...].astype(f32)
    ranks = down_ref.shape[0]
    raw_low, g_low = low_all[:, :ranks], low_all[:, ranks:]
    jobs = len_ref.shape[1]
    position = core * count + lax.broadcasted_iota(jnp.int32, (count, ranks), 0)
    owner = jnp.zeros((count, ranks), jnp.int32)
    end = jnp.zeros((1, 1), jnp.int32)
    for j in range(jobs):
        end = end + len_ref[0:1, j:j + 1]
        owner = owner + (end <= position).astype(jnp.int32)
    mask = (
        owner == lax.broadcasted_iota(jnp.int32, (count, ranks), 1) // (ranks // jobs)
    ).astype(f32)
    low = (raw_low * scale * mask).astype(bf16)
    d_low = (ADAPTER_SCALE * g_low * mask).astype(bf16)
    gain = gain_ref[:, pl.ds(pl.multiple_of(me * width, LANES), width)]
    normed = (x * scale * gain).astype(bf16)
    pd_ref[...] = lax.dot_general(d_low, normed, FIRST, preferred_element_type=f32)
    pu_ref[...] = ADAPTER_SCALE * lax.dot_general(low, g_ref[...], FIRST, preferred_element_type=f32)
    shared.append(send(pd_ref, ppd, qs, qr, 1, partner))
    shared.append(send(pu_ref, ppu, qs, qr, 2, partner))

    def share(k):
        expert = peers[k] // per
        gate, sign = jnp.zeros((count, 1), f32), jnp.zeros((count, 1), f32)
        for e in range(experts):
            mark = (expert == e).astype(f32)
            gate += mark * column(e)
            sign += mark * column(8 + e)
        return select_ref[expert], gate, sign

    spread = jnp.zeros((count, 1), f32)
    stat = jnp.zeros((count, 1), f32)
    for copy in told:
        copy.wait()
    for k in range(n):
        chosen, gate, sign = share(k)
        terms = vsend[...] if k == 0 else vec_in[k - 1]
        picked = lax.dot_general(chosen, terms, FIRST, preferred_element_type=f32)
        spread = spread + sign * (picked[:, 0:1] + picked[:, 2:3])
        stat = stat + gate * (picked[:, 1:2] + picked[:, 3:4])
    delta = spread * delta_of
    low_stat = jnp.sum(d_low.astype(f32) * raw_low, axis=1, keepdims=True)
    stat = stat / scale + low_stat + delta * raw_spread
    total = jnp.dot(d_low, down_ref[...], preferred_element_type=f32)
    router = router_ref[:, pl.ds(pl.multiple_of(me * width, LANES), width)].astype(f32)
    for e in range(experts):
        total = total + (delta * column(8 + e)) * router[e:e + 1, :]
    out_ref[...] = g_ref[...].astype(f32) + scale * (total * gain) - x * (
        scale * scale * scale * stat / (n * width)
    )

    def add(k, block):
        chosen, gate, _ = share(k)
        picked = lax.dot_general(chosen, block, FIRST, preferred_element_type=f32)
        return out_ref[...] + (gate * scale) * gain * picked

    finish(0)
    out_ref[...] = add(0, sendbuf[0])
    for k in order[:-2]:
        sent[k].wait()
        out_ref[...] = add(k, landing[k - 1])
    last = order[-2]
    sent[last].wait_recv()
    result[...] = add(last, landing[last - 1]).astype(bf16)
    handed = send(result, back_out, zs, zr, 0, ahead)
    sent[last].wait_send()
    for k in range(1, n):
        xs[k].wait_send()
        gs[k].wait_send()
    shared[1].wait()
    pd_out[...] = pd_ref[...] + ppd[...]
    shared[2].wait()
    pu_out[...] = pu_ref[...] + ppu[...]
    handed.wait()


def settle_kernel(*refs):
    half = len(refs) // 2
    for src, dst in zip(refs[:half], refs[half:]):
        dst[...] = src[...]


def tick(n, per, shards, sections, x, g, routes, lengths, gains, router, down, up, wg, wu, wd):
    count, width = x.shape
    experts = router.shape[0]
    hidden = wg.shape[2]
    ranks = down.shape[0]
    slots = shards * CAP
    f32, bf16 = jnp.float32, jnp.bfloat16
    vmem = pl.BlockSpec(memory_space=pltpu.VMEM)
    hbm = pl.BlockSpec(memory_space=pl.ANY)
    dma = pltpu.SemaphoreType.DMA
    outs = (
        jax.ShapeDtypeStruct((count, width), bf16),
        jax.ShapeDtypeStruct((ranks, width), f32),
        jax.ShapeDtypeStruct((ranks, width), f32),
    )
    values = pl.pallas_call(
        functools.partial(tick_kernel, n, per, experts, sections),
        out_shape=outs,
        in_specs=[vmem] * 8 + [hbm] * 3,
        out_specs=(vmem,) * 3,
        scratch_shapes=[
            pltpu.VMEM((n, width, hidden), bf16),
            pltpu.VMEM((n, width, hidden), bf16),
            pltpu.VMEM((n, hidden, width), bf16),
            pltpu.VMEM((n, slots, width), bf16),
            pltpu.VMEM((n, slots, width), bf16),
            pltpu.VMEM((experts, CAP, width), bf16),
            pltpu.VMEM((experts, CAP, width), bf16),
            pltpu.VMEM((experts, CAP, count), bf16),
            pltpu.VMEM((8, count), f32),
            pltpu.VMEM((count, 2 * ranks), bf16),
            pltpu.VMEM((n - 1, 8, count), f32),
            pltpu.VMEM((n - 1, count, 2 * ranks), bf16),
            pltpu.VMEM((slots, hidden), f32),
            pltpu.VMEM((slots, hidden), f32),
            pltpu.VMEM((slots, hidden), f32),
            pltpu.VMEM((slots, hidden), bf16),
            pltpu.VMEM((slots, hidden), bf16),
            pltpu.VMEM((slots, LANES), f32),
            pltpu.VMEM((slots, LANES), f32),
            pltpu.VMEM((slots, LANES), f32),
            pltpu.VMEM((slots, LANES), f32),
            pltpu.VMEM((n, slots, width), f32),
            pltpu.VMEM((n, CAP, width), f32),
            pltpu.VMEM((CAP, LANES), f32),
            pltpu.VMEM((CAP, LANES), bf16),
            pltpu.VMEM((n - 1, CAP, LANES), bf16),
            pltpu.VMEM((ranks, width), f32),
            pltpu.VMEM((ranks, width), f32),
            pltpu.VMEM((ranks, width), f32),
            pltpu.VMEM((ranks, width), f32),
            pltpu.VMEM((n, CAP, width), bf16),
            pltpu.VMEM((n - 1, CAP, width), bf16),
            pltpu.VMEM((count, width), f32),
            pltpu.VMEM((count, width), bf16),
            pltpu.VMEM((LANES, count), f32),
            dma((n, 3)),
            *[dma((n - 1,))] * 4, *[dma((n,))] * 4, *[dma((n - 1,))] * 4,
            dma((2,)), dma((3,)), dma((3,)), *[dma((n - 1,))] * 2, *[dma((n,))] * 2,
            *[dma((n - 1,))] * 2, dma((1,)), dma((1,)),
        ],
        compiler_params=pltpu.CompilerParams(
            collective_id=0, has_side_effects=True, vmem_limit_bytes=VMEM_LIMIT
        ),
    )(x, g, routes, lengths, gains, router, down, up, wg, wu, wd)
    return pl.pallas_call(
        settle_kernel, out_shape=outs, in_specs=[vmem] * 3, out_specs=(vmem,) * 3
    )(*values)


def body(
    stash,
    cotangent,
    backward_expert_routes,
    backward_job_lengths,
    layer_norm_gains,
    router,
    expert_gate_weight,
    expert_up_weight,
    expert_down_weight,
    adapter_down_maps,
    adapter_up_maps,
):
    n = lax.axis_size("expert")
    shards = lax.axis_size("dp")
    sections = lax.axis_size("section")
    per = n // router.shape[2]
    handed_back, down_grad, up_grad = tick(
        n, per, shards, sections, stash[0], cotangent[0], backward_expert_routes[0].T,
        backward_job_lengths, layer_norm_gains, router[0].T, adapter_down_maps[0].T,
        adapter_up_maps[0], expert_gate_weight, expert_up_weight, expert_down_weight,
    )
    return (handed_back[None], down_grad.T[None], up_grad[None])


def solution(mesh):
    return jax.shard_map(
        body,
        mesh=mesh,
        in_specs=(
            P("section", "dp", "expert"),
            P("section", "dp", "expert"),
            P("section", "dp", None),
            P("section", None),
            P("section", None),
            P("section", None, None),
            P("section", None, ("expert", "dp")),
            P("section", None, ("expert", "dp")),
            P("section", ("expert", "dp"), None),
            P("section", "expert", None),
            P("section", None, "expert"),
        ),
        out_specs=(
            P("section", "dp", "expert"),
            P("section", "expert", None),
            P("section", None, "expert"),
        ),
        check_vma=False,
    )
```

```python
import functools

import jax
import jax.numpy as jnp
from jax import lax
from jax.experimental import pallas as pl
from jax.experimental.pallas import tpu as pltpu
from jax.sharding import PartitionSpec as P

CAP = 80

EPS = 1e-05
ADAPTER_SCALE = 0.5
MESH = pl.DeviceIdType.MESH
VMEM_LIMIT = 62 * 1024 * 1024
LANES = 128
DEPTH = 6
TILES = (1792, 896, 512, 256, 128)
ACT_TILES = (512, 256, 128)
LAST = (((1,), (1,)), ((), ()))
FIRST = (((0,), (0,)), ((), ()))


def paired(me, k, n):
    out, bit = me, 1
    while bit < n:
        if k & bit:
            out = out + bit * (1 - 2 * lax.rem(me // bit, 2))
        bit *= 2
    return out


def tick_kernel(
    n, per, experts, sections,
    x_ref, g_ref, route_ref, len_ref, gain_ref, router_ref, down_ref, up_ref, wg_hbm, wu_hbm, wd_hbm,
    back_out, pd_out, pu_out,
    wg_v, wu_v, wd_v, xs_in, gs_in, xs_ref, gs_ref, select_ref, stats_ref, lows_ref, stats_in, lows_in,
    gate_acc, up_acc, back_acc, dg_ref, du_ref, ssq, gsum, ssum, vec_ref, dn_ref, dn_own,
    pdn, pdn_own, pvec, vsend, vec_in, pd_ref, pu_ref, ppd, ppu, sendbuf, landing, out_ref, result, turn,
    ws, xs_s, xs_r, gs_s, gs_r, xfs, xfr, gfs, gfr, ss, sr, ls, lr, own, qs, qr, vs, vr, ps, pr,
    es, er, os, ox, zs, zr,
):
    me = lax.axis_index("expert")
    core = lax.axis_index("dp")
    sec = lax.axis_index("section")
    other = 1 - core
    partner = {"dp": other}
    ahead = {"section": lax.rem(sec + sections - 1, sections)}
    behind = {"section": lax.rem(sec + 1, sections)}
    peers = [paired(me, k, n) for k in range(n)]
    count, width = x_ref.shape
    cap = select_ref.shape[1]
    hidden = wg_v.shape[2]
    f32, bf16 = jnp.float32, jnp.bfloat16

    def weights(k):
        cols = pl.ds(pl.multiple_of(peers[k] * width, LANES), width)
        return [
            pltpu.make_async_copy(wg_hbm.at[0, cols, :], wg_v.at[k], ws.at[k, 0]),
            pltpu.make_async_copy(wu_hbm.at[0, cols, :], wu_v.at[k], ws.at[k, 1]),
            pltpu.make_async_copy(wd_hbm.at[0, :, cols], wd_v.at[k], ws.at[k, 2]),
        ]

    inner = list(range(1, n - 1))
    groups = [inner[i:i + 2] for i in range(0, len(inner), 2)] + [[n - 1]]
    blocks_of = [weights(k) for k in range(n)]
    loads = list(blocks_of[0])
    for group in groups:
        loads += [blocks_of[k][i] for k in group for i in (0, 1)] + [blocks_of[k][2] for k in group]
    for copy in loads[:DEPTH]:
        copy.start()
    loaded = [0]

    def load(count):
        for _ in range(count):
            loads[loaded[0]].wait()
            if loaded[0] + DEPTH < len(loads):
                loads[loaded[0] + DEPTH].start()
            loaded[0] += 1

    neighbours = [{"expert": peer} for peer in peers[1:]] + [partner, ahead, behind]
    barrier = pltpu.get_barrier_semaphore()
    for target in neighbours:
        pl.semaphore_signal(barrier, inc=1, device_id=target, device_id_type=MESH)

    def send(src, dst, a, b, k, target):
        copy = pltpu.make_async_remote_copy(
            src_ref=src, dst_ref=dst, send_sem=a.at[k], recv_sem=b.at[k],
            device_id=target, device_id_type=MESH,
        )
        copy.start()
        return copy

    line = lax.broadcasted_iota(jnp.int32, (8, count), 0)
    first = (route_ref[0:1, :] == line).astype(f32)
    second = (route_ref[1:2, :] == line).astype(f32)
    member = first + second
    before = (
        lax.broadcasted_iota(jnp.int32, (count, count), 0)
        < lax.broadcasted_iota(jnp.int32, (count, count), 1)
    ).astype(bf16)
    rank = jnp.dot(member.astype(bf16), before, preferred_element_type=f32)
    place = jnp.where(member > 0, rank, -1.0)
    slot = lax.broadcasted_iota(jnp.int32, (cap, count), 0).astype(f32)
    x, g = x_ref[...], g_ref[...]
    for e in range(experts):
        chosen = (place[e:e + 1, :] == slot).astype(bf16)
        select_ref[e] = chosen
        xs_ref[e] = jnp.dot(chosen, x, preferred_element_type=f32).astype(bf16)
        gs_ref[e] = jnp.dot(chosen, g, preferred_element_type=f32).astype(bf16)

    pl.semaphore_wait(barrier, len(neighbours))
    mine = pl.ds(pl.multiple_of(core * cap, 16), cap)
    home = me // per
    xs_on = [send(xs_ref.at[home], xs_in.at[0, mine], xfs, xfr, 0, partner)]
    gs_on = [send(gs_ref.at[home], gs_in.at[0, mine], gfs, gfr, 0, partner)]
    xs, gs = {}, {}
    for group in groups:
        for k in group:
            xs[k] = send(
                xs_ref.at[peers[k] // per], xs_in.at[k, mine], xs_s, xs_r, k - 1, {"expert": peers[k]}
            )
        for k in group:
            gs[k] = send(
                gs_ref.at[peers[k] // per], gs_in.at[k, mine], gs_s, gs_r, k - 1, {"expert": peers[k]}
            )
    kept = [
        pltpu.make_async_copy(xs_ref.at[home], xs_in.at[0, mine], own.at[0]),
        pltpu.make_async_copy(gs_ref.at[home], gs_in.at[0, mine], own.at[1]),
    ]
    for copy in kept:
        copy.start()

    xf = x.astype(f32)
    features = pl.ds(pl.multiple_of(me * width, LANES), width)
    gained = (xf * gain_ref[:, features]).astype(bf16)
    router = jnp.concatenate(
        [router_ref[:, features].astype(f32), jnp.zeros((8 - experts, width), f32)], axis=0
    )
    raw = lax.dot_general(router.astype(bf16), gained, LAST, preferred_element_type=f32)
    square = lax.dot_general(
        jnp.ones((8, width), f32), xf * xf, LAST,
        precision=lax.Precision.HIGHEST, preferred_element_type=f32,
    )
    stats_ref[...] = jnp.where(line < experts, raw, square)
    lows_ref[...] = jnp.concatenate(
        [
            lax.dot_general(gained, down_ref[...], LAST, preferred_element_type=f32),
            lax.dot_general(g, up_ref[...], LAST, preferred_element_type=f32),
        ],
        axis=1,
    ).astype(bf16)
    small = []
    for k in range(1, n):
        target = {"expert": peers[k]}
        small.append(send(stats_ref, stats_in.at[k - 1], ss, sr, k - 1, target))
        small.append(send(lows_ref, lows_in.at[k - 1], ls, lr, k - 1, target))

    def pass_on(group, arrived, buffer, onward, a, b):
        for k in group:
            arrived[k].wait_recv()
            landed = buffer.at[k, mine]
            onward.append(send(landed, landed, a, b, k, partner))

    pass_x = lambda group: pass_on(group, xs, xs_in, xs_on, xfs, xfr)
    pass_g = lambda group: pass_on(group, gs, gs_in, gs_on, gfs, gfr)

    tile = next(t for t in TILES if hidden % t == 0)

    def add_to(acc, k, c, p):
        if k == 0:
            acc[:, c] = p
        else:
            acc[:, c] += p

    def scaled(k):
        xs_on[k].wait()
        xk = xs_in[k].astype(f32)
        part = jnp.sum(xk * xk, axis=1, keepdims=True)
        if k == 0:
            ssq[...] = jnp.broadcast_to(part, ssq.shape)
        else:
            ssq[...] += part
        features = pl.ds(pl.multiple_of(peers[k] * width, LANES), width)
        return (xk * gain_ref[:, features]).astype(bf16)

    def forth(k):
        load(2)
        xk = scaled(k)
        for t in range(hidden // tile):
            c = slice(t * tile, (t + 1) * tile)
            add_to(gate_acc, k, c, jnp.dot(xk, wg_v[k, :, c], preferred_element_type=f32))
            add_to(up_acc, k, c, jnp.dot(xk, wu_v[k, :, c], preferred_element_type=f32))

    def back_from(k):
        load(1)
        gs_on[k].wait()
        for t in range(hidden // tile):
            c = slice(t * tile, (t + 1) * tile)
            add_to(back_acc, k, c, lax.dot_general(
                gs_in[k], wd_v[k, c, :], LAST, preferred_element_type=f32
            ))

    for copy in kept:
        copy.wait()
    forth(0)
    back_from(0)
    pass_x(groups[0])
    for i, group in enumerate(groups[:-1]):
        for j, k in enumerate(group):
            forth(k)
            if j == 0:
                pass_g(group)
        pass_x(groups[i + 1])
        for k in group:
            back_from(k)
    k = n - 1
    pass_g(groups[-1])
    load(2)
    xk = scaled(k)
    load(1)
    gs_on[k].wait()
    scale = lax.rsqrt(ssq[:, 0:1] / (n * width) + EPS)
    gk = gs_in[k]
    gate_sum = jnp.zeros(gsum.shape, f32)
    stat_sum = jnp.zeros(gsum.shape, f32)
    act_tile = next(t for t in ACT_TILES if hidden % t == 0)
    for t in range(hidden // act_tile):
        c = slice(t * act_tile, (t + 1) * act_tile)
        gate = jnp.dot(xk, wg_v[k, :, c], preferred_element_type=f32)
        up = jnp.dot(xk, wu_v[k, :, c], preferred_element_type=f32)
        back = lax.dot_general(gk, wd_v[k, c, :], LAST, preferred_element_type=f32)
        gate = (gate + gate_acc[:, c]) * scale
        up = (up + up_acc[:, c]) * scale
        back = back + back_acc[:, c]
        sig = jax.nn.sigmoid(gate)
        act = gate * sig
        both = back * up
        d_gate = both * (sig + act * (1.0 - sig))
        dg_ref[:, c] = d_gate.astype(bf16)
        du_ref[:, c] = (back * act).astype(bf16)
        p, q = both * act, d_gate * gate
        for j in range(act_tile // LANES):
            l = slice(j * LANES, (j + 1) * LANES)
            gate_sum += p[:, l]
            stat_sum += q[:, l]
    gsum[...] = gate_sum
    ssum[...] = stat_sum
    theirs = pl.ds(pl.multiple_of(other * cap, 8), cap)
    ours = pl.ds(pl.multiple_of(core * cap, 8), cap)

    sub = next(t for t in (256, 128) if width % t == 0)
    parts = [slice(j * sub, (j + 1) * sub) for j in range(width // sub)]
    units = [(k, j) for j in range(len(parts)) for k in range(n - 1, 0, -1)]
    pairs = [units[i:i + 2] for i in range(0, len(units), 2)]
    shared, halves, sent, told = [], {}, {}, []

    def exchange(k, j):
        halves[k, j] = send(
            dn_ref.at[k, j, theirs], pdn.at[k, j], ps, pr, k * len(parts) + j, partner
        )

    def finish(k, j):
        halves[k, j].wait()
        sendbuf[k, j] = (dn_ref[k, j, ours, :] + pdn[k, j]).astype(bf16)
        sent[k, j] = send(
            sendbuf.at[k, j], landing.at[k - 1, j], es, er, (k - 1) * len(parts) + j,
            {"expert": peers[k]},
        )

    def tell():
        shared[0].wait()
        v = vec_ref[ours, :] + pvec[...]
        high = v.astype(bf16)
        rest = (v - high.astype(f32)).astype(bf16)
        lane = lax.broadcasted_iota(jnp.int32, v.shape, 1)
        vsend[...] = jnp.where(lane < 2, high.astype(f32), rest.astype(f32)).astype(bf16)
        for k in range(1, n):
            told.append(send(vsend, vec_in.at[k - 1], vs, vr, k - 1, {"expert": peers[k]}))

    def product(d_ref, w_ref, k, j):
        return lax.dot_general(d_ref[...], w_ref[k, parts[j], :], LAST, preferred_element_type=f32)

    def region(pair):
        for k, j in pair:
            dn_ref[k, j] = product(dg_ref, wg_v, k, j) + product(du_ref, wu_v, k, j)

    region(pairs[0])
    total = jnp.sum(gsum[...], axis=1, keepdims=True)
    lane = lax.broadcasted_iota(jnp.int32, gsum.shape, 1)
    vec_ref[...] = jnp.where(
        lane % 2 == 0, total, total + jnp.sum(ssum[...], axis=1, keepdims=True)
    )
    shared.append(send(vec_ref.at[theirs], pvec, qs, qr, 0, partner))
    for unit in pairs[0]:
        exchange(*unit)
    for copy in small:
        copy.wait()
    for pair in pairs[1:2]:
        region(pair)
    stat_rows, low_all = stats_ref[...], lows_ref[...].astype(f32)
    for k in range(1, n):
        stat_rows = stat_rows + stats_in[k - 1]
        low_all = low_all + lows_in[k - 1].astype(f32)
    scale_row = lax.rsqrt(stat_rows[experts:experts + 1, :] / (n * width) + EPS)
    sign_rows = first - second
    spread_row = jnp.sum(
        jnp.where(line < experts, sign_rows * stat_rows, 0.0), axis=0, keepdims=True
    )
    upper = jax.nn.sigmoid(spread_row * scale_row)
    turn[...] = jnp.zeros_like(turn)
    turn[0:8, :] = upper * first + (1.0 - upper) * second
    turn[8:16, :] = sign_rows
    turn[16:17, :] = upper * (1.0 - upper)
    turn[17:18, :] = scale_row
    turn[18:19, :] = spread_row
    token = turn[...].T
    column = lambda i: token[:, i:i + 1]
    delta_of, scale, raw_spread = column(16), column(17), column(18)
    x = x_ref[...].astype(f32)
    ranks = down_ref.shape[0]
    raw_low, g_low = low_all[:, :ranks], low_all[:, ranks:]
    jobs = len_ref.shape[1]
    position = core * count + lax.broadcasted_iota(jnp.int32, (count, ranks), 0)
    owner = jnp.zeros((count, ranks), jnp.int32)
    end = jnp.zeros((1, 1), jnp.int32)
    for j in range(jobs):
        end = end + len_ref[0:1, j:j + 1]
        owner = owner + (end <= position).astype(jnp.int32)
    mask = (
        owner == lax.broadcasted_iota(jnp.int32, (count, ranks), 1) // (ranks // jobs)
    ).astype(f32)
    low = (raw_low * scale * mask).astype(bf16)
    d_low = (ADAPTER_SCALE * g_low * mask).astype(bf16)
    gain = gain_ref[:, pl.ds(pl.multiple_of(me * width, LANES), width)]
    normed = (x * scale * gain).astype(bf16)
    pd_ref[...] = lax.dot_general(d_low, normed, FIRST, preferred_element_type=f32)
    pu_ref[...] = ADAPTER_SCALE * lax.dot_general(low, g_ref[...], FIRST, preferred_element_type=f32)
    for i, pair in enumerate(pairs[1:]):
        if i:
            region(pair)
        for unit in pair:
            exchange(*unit)
        if i == 0:
            tell()
            shared.append(send(pd_ref, ppd, qs, qr, 1, partner))
            shared.append(send(pu_ref, ppu, qs, qr, 2, partner))
        for unit in pairs[i]:
            finish(*unit)
    for copy in told:
        copy.wait()

    def own_region(j):
        dn_ref[0, j] = product(dg_ref, wg_v, 0, j)
        dn_own[j] = product(du_ref, wu_v, 0, j)

    def own_exchange(j):
        exchange(0, j)
        halves[-1, j] = send(dn_own.at[j, theirs], pdn_own.at[j], os, ox, j, partner)

    def own_finish(j):
        halves[0, j].wait()
        halves[-1, j].wait()
        sendbuf[0, j] = (
            (dn_ref[0, j, ours, :] + dn_own[j, ours, :]) + (pdn[0, j] + pdn_own[j])
        ).astype(bf16)

    own_region(0)
    def share(k):
        expert = peers[k] // per
        gate, sign = jnp.zeros((count, 1), f32), jnp.zeros((count, 1), f32)
        for e in range(experts):
            mark = (expert == e).astype(f32)
            gate += mark * column(e)
            sign += mark * column(8 + e)
        return select_ref[expert], gate, sign

    gates = {}
    spread = jnp.zeros((count, 1), f32)
    stat = jnp.zeros((count, 1), f32)
    for k in range(n):
        chosen, gate, sign = share(k)
        gates[k] = gate * scale
        terms = vsend[...] if k == 0 else vec_in[k - 1]
        picked = lax.dot_general(chosen, terms, FIRST, preferred_element_type=f32)
        spread = spread + sign * (picked[:, 0:1] + picked[:, 2:3])
        stat = stat + gate * (picked[:, 1:2] + picked[:, 3:4])
    delta = spread * delta_of
    low_stat = jnp.sum(d_low.astype(f32) * raw_low, axis=1, keepdims=True)
    stat = stat / scale + low_stat + delta * raw_spread
    total = jnp.dot(d_low, down_ref[...], preferred_element_type=f32)
    router = router_ref[:, pl.ds(pl.multiple_of(me * width, LANES), width)].astype(f32)
    for e in range(experts):
        total = total + (delta * column(8 + e)) * router[e:e + 1, :]
    out_ref[...] = g_ref[...].astype(f32) + scale * (total * gain) - x * (
        scale * scale * scale * stat / (n * width)
    )


    own_exchange(0)
    for unit in pairs[-1]:
        finish(*unit)
    for j in range(1, len(parts)):
        own_region(j)
        own_exchange(j)
    handed = []
    for j, c in enumerate(parts):
        own_finish(j)
        for k in range(n - 1, 0, -1):
            sent[k, j].wait_recv()
        out = out_ref[:, c]
        for k in range(n):
            block = landing[k - 1, j] if k else sendbuf[0, j]
            picked = lax.dot_general(
                select_ref[peers[k] // per], block, FIRST, preferred_element_type=f32
            )
            out = out + gates[k] * gain[:, c] * picked
        result[j] = out.astype(bf16)
        handed.append(send(result.at[j], back_out.at[:, c], zs, zr, j, ahead))
    for copy in sent.values():
        copy.wait_send()
    for k in range(1, n):
        xs[k].wait_send()
        gs[k].wait_send()
    shared[1].wait()
    pd_out[...] = pd_ref[...] + ppd[...]
    shared[2].wait()
    pu_out[...] = pu_ref[...] + ppu[...]
    for copy in handed:
        copy.wait()


def settle_kernel(*refs):
    half = len(refs) // 2
    for src, dst in zip(refs[:half], refs[half:]):
        dst[...] = src[...]


def tick(n, per, shards, sections, x, g, routes, lengths, gains, router, down, up, wg, wu, wd):
    count, width = x.shape
    experts = router.shape[0]
    hidden = wg.shape[2]
    ranks = down.shape[0]
    slots = shards * CAP
    sub = next(t for t in (256, 128) if width % t == 0)
    parts = width // sub
    f32, bf16 = jnp.float32, jnp.bfloat16
    vmem = pl.BlockSpec(memory_space=pltpu.VMEM)
    hbm = pl.BlockSpec(memory_space=pl.ANY)
    dma = pltpu.SemaphoreType.DMA
    outs = (
        jax.ShapeDtypeStruct((count, width), bf16),
        jax.ShapeDtypeStruct((ranks, width), f32),
        jax.ShapeDtypeStruct((ranks, width), f32),
    )
    values = pl.pallas_call(
        functools.partial(tick_kernel, n, per, experts, sections),
        out_shape=tuple(pltpu.VMEM(o.shape, o.dtype) for o in outs),
        in_specs=[vmem] * 8 + [hbm] * 3,
        out_specs=(vmem,) * 3,
        scratch_shapes=[
            pltpu.VMEM((n, width, hidden), bf16),
            pltpu.VMEM((n, width, hidden), bf16),
            pltpu.VMEM((n, hidden, width), bf16),
            pltpu.VMEM((n, slots, width), bf16),
            pltpu.VMEM((n, slots, width), bf16),
            pltpu.VMEM((experts, CAP, width), bf16),
            pltpu.VMEM((experts, CAP, width), bf16),
            pltpu.VMEM((experts, CAP, count), bf16),
            pltpu.VMEM((8, count), f32),
            pltpu.VMEM((count, 2 * ranks), bf16),
            pltpu.VMEM((n - 1, 8, count), f32),
            pltpu.VMEM((n - 1, count, 2 * ranks), bf16),
            pltpu.VMEM((slots, hidden), f32),
            pltpu.VMEM((slots, hidden), f32),
            pltpu.VMEM((slots, hidden), f32),
            pltpu.VMEM((slots, hidden), bf16),
            pltpu.VMEM((slots, hidden), bf16),
            pltpu.VMEM((slots, LANES), f32),
            pltpu.VMEM((slots, LANES), f32),
            pltpu.VMEM((slots, LANES), f32),
            pltpu.VMEM((slots, LANES), f32),
            pltpu.VMEM((n, parts, slots, sub), f32),
            pltpu.VMEM((parts, slots, sub), f32),
            pltpu.VMEM((n, parts, CAP, sub), f32),
            pltpu.VMEM((parts, CAP, sub), f32),
            pltpu.VMEM((CAP, LANES), f32),
            pltpu.VMEM((CAP, LANES), bf16),
            pltpu.VMEM((n - 1, CAP, LANES), bf16),
            pltpu.VMEM((ranks, width), f32),
            pltpu.VMEM((ranks, width), f32),
            pltpu.VMEM((ranks, width), f32),
            pltpu.VMEM((ranks, width), f32),
            pltpu.VMEM((n, parts, CAP, sub), bf16),
            pltpu.VMEM((n - 1, parts, CAP, sub), bf16),
            pltpu.VMEM((count, width), f32),
            pltpu.VMEM((parts, count, sub), bf16),
            pltpu.VMEM((LANES, count), f32),
            dma((n, 3)),
            *[dma((n - 1,))] * 4, *[dma((n,))] * 4, *[dma((n - 1,))] * 4,
            dma((2,)), dma((3,)), dma((3,)), *[dma((n - 1,))] * 2, *[dma((n * parts,))] * 2,
            *[dma(((n - 1) * parts,))] * 2, *[dma((parts,))] * 4,
        ],
        compiler_params=pltpu.CompilerParams(
            collective_id=0, has_side_effects=True, vmem_limit_bytes=VMEM_LIMIT
        ),
    )(x, g, routes, lengths, gains, router, down, up, wg, wu, wd)
    return pl.pallas_call(
        settle_kernel, out_shape=outs, in_specs=[vmem] * 3, out_specs=(vmem,) * 3
    )(*[pltpu.with_memory_space_constraint(v, pltpu.VMEM) for v in values])


def body(
    stash,
    cotangent,
    backward_expert_routes,
    backward_job_lengths,
    layer_norm_gains,
    router,
    expert_gate_weight,
    expert_up_weight,
    expert_down_weight,
    adapter_down_maps,
    adapter_up_maps,
):
    n = lax.axis_size("expert")
    shards = lax.axis_size("dp")
    sections = lax.axis_size("section")
    per = n // router.shape[2]
    handed_back, down_grad, up_grad = tick(
        n, per, shards, sections, stash[0], cotangent[0], backward_expert_routes[0].T,
        backward_job_lengths, layer_norm_gains, router[0].T, adapter_down_maps[0].T,
        adapter_up_maps[0], expert_gate_weight, expert_up_weight, expert_down_weight,
    )
    return (handed_back[None], down_grad.T[None], up_grad[None])


def solution(mesh):
    return jax.shard_map(
        body,
        mesh=mesh,
        in_specs=(
            P("section", "dp", "expert"),
            P("section", "dp", "expert"),
            P("section", "dp", None),
            P("section", None),
            P("section", None),
            P("section", None, None),
            P("section", None, ("expert", "dp")),
            P("section", None, ("expert", "dp")),
            P("section", ("expert", "dp"), None),
            P("section", "expert", None),
            P("section", None, "expert"),
        ),
        out_specs=(
            P("section", "dp", "expert"),
            P("section", "expert", None),
            P("section", None, "expert"),
        ),
        check_vma=False,
    )
```
